32 devices in a mesh: grp: 4 (over y, x), node: 8 (over z, core).
Axes of the slice: x: 2, y: 2, z: 4, core: 2. Of those that a mesh axis runs over, the one named last changes fastest.
Arguments:
- damage: bfloat16 [1024, 16384], P('grp', 'node'), may hold values from -6 to 6
- basis_table: bfloat16 [1024, 512], P('grp'), may hold values from -6 to 6
- train_ids: int32 [1024], P('grp'), may hold values from 0 to 1023, each once
- counts: int32 [4], replicated, may hold values from 64 to 256
- new_table: bfloat16 [512, 512], replicated, may hold values from -6 to 6
- new_ids: int32 [256], replicated, may hold values from 0 to 511
Outputs:
- surrogate: bfloat16 [256, 16384], P('grp', 'node')
- peak: float32 [256], P('grp')
- spread: float32 [256], P('grp')
The draws below stay inside these ranges and needn't reach their ends.
Inputs may be any that keep to these rules, and one draw needn't show every extreme that they name: `train_ids`: each row of basis_table is named by exactly one slot.
All inputs are finite; a program needn't handle non-finite values.
Results may differ from the reference program's by a relative error of at most 0.0085.
Values may be sent and summed in bfloat16 or wider, within the bound.
No kernel may reach another device: no remote copies, remote signals or barrier semaphores. Data moves between devices by JAX's collectives and lax.ppermute only.
A program may use at most 64 MiB of HBM per device.

```python
import jax
import jax.numpy as jnp
from jax import lax

TERMS = 512
SLOT = 256
NODE_DEV = 2048
GROUPS = 4
SAMPLES = 1024
NODES = 16384
NEW_SAMPLES = 256
NEW_TABLE_ROWS = 512
N_NODE = 8


def touch_ends(values, rng, least, largest):
    extent = values.shape
    spot = [jax.random.randint(jax.random.fold_in(rng, axis), (), 0, extent[axis]) for axis in range(len(extent))]
    values = values.at[tuple(spot)].set(least)
    longest = extent.index(max(extent))
    spot[longest] = (spot[longest] + 1) % extent[longest]
    return values.at[tuple(spot)].set(largest)


def block_levels(rng, shape, pieces, least, top_value):
    level, own = 1.0, jax.random.fold_in(rng, 6)
    for position, blocks in pieces:
        draws = jnp.exp(jax.random.uniform(jax.random.fold_in(own, position), (blocks,), jnp.float32, least / len(pieces), top_value / len(pieces)))
        level = level * jnp.repeat(draws, shape[position] // blocks).reshape([-1 if axis == position else 1 for axis in range(len(shape))])
    return level


def centred(rng, extent, scale, limit, cuts=(), kind=jnp.bfloat16):
    loudness = block_levels(rng, extent, cuts, -0.22, 0.18) if cuts else 1.0
    drawn = jax.random.normal(rng, extent, jnp.float32) * scale * loudness
    return jnp.minimum(jnp.maximum(drawn, -limit), limit).astype(kind)


def setup_inputs(seed: int = 0) -> dict:
    key_list = jax.random.split(jax.random.key(seed), 7)
    damage = centred(key_list[0], (SAMPLES, NODES), 1.0, 6.0, ((0, 4), (1, 8)))
    basis_table = centred(key_list[1], (SAMPLES, TERMS), 1.0, 6.0, ((0, 4),))
    train_ids = jax.random.permutation(key_list[2], SAMPLES).astype(jnp.int32)
    counts = touch_ends(jax.random.randint(key_list[3], (GROUPS,), SLOT // 4, SLOT + 1), jax.random.fold_in(key_list[3], 1), SLOT // 4, SLOT).astype(jnp.int32)
    new_table = centred(key_list[4], (NEW_TABLE_ROWS, TERMS), 1.0, 6.0)
    new_ids = touch_ends(jax.random.randint(key_list[5], (NEW_SAMPLES,), 0, NEW_TABLE_ROWS), jax.random.fold_in(key_list[5], 1), 0, NEW_TABLE_ROWS - 1).astype(jnp.int32)
    return {"damage": damage, "basis_table": basis_table, "train_ids": train_ids, "counts": counts, "new_table": new_table, "new_ids": new_ids}


def reference(damage, basis_table, train_ids, counts, new_table, new_ids):
    slot_index = jnp.arange(SAMPLES, dtype=jnp.int32)
    live_slot = slot_index % SLOT < counts[slot_index // SLOT]
    sample_total = jnp.sum(counts).astype(jnp.float32)
    chosen = jnp.take(basis_table, train_ids, axis=0)
    weighted = jnp.where(live_slot[:, None], chosen, jnp.zeros_like(chosen)).astype(jnp.float32)
    new_rows = jnp.take(new_table, new_ids, axis=0).astype(jnp.float32)

    def one_block(block_index):
        offset = (block_index * NODE_DEV).astype(jnp.int32)
        block_data = lax.dynamic_slice_in_dim(damage, offset, NODE_DEV, 1).astype(jnp.float32)
        coef_full = jnp.dot(weighted.T, block_data, precision=lax.Precision.HIGHEST) / sample_total
        coef_half = lax.optimization_barrier(coef_full.astype(jnp.bfloat16)).astype(jnp.float32)
        values = jnp.dot(new_rows, coef_half, precision=lax.Precision.HIGHEST)
        return (values.astype(jnp.bfloat16), lax.optimization_barrier(jnp.max(values, axis=1)), lax.optimization_barrier(jnp.sum(values * values, axis=1)))
    fields, peaks, squares = lax.map(one_block, jnp.arange(N_NODE, dtype=jnp.int32))
    surrogate = jnp.transpose(fields, (1, 0, 2)).reshape(NEW_SAMPLES, NODES)
    peak = lax.optimization_barrier(jnp.max(peaks, axis=0))
    spread = jnp.sqrt(lax.optimization_barrier(jnp.sum(squares, axis=0)) / NODES + 1e-06)
    return (surrogate, peak, spread)
```

```python
import functools

import jax
import jax.numpy as jnp
from jax import lax
from jax.experimental import pallas as pl
from jax.experimental.pallas import tpu as pltpu
from jax.sharding import PartitionSpec as P


FULL = pl.BlockSpec(memory_space=pltpu.VMEM)
SCALAR = pl.BlockSpec(memory_space=pltpu.SMEM)


def mate(index, step, size):
    return index ^ step if size & (size - 1) == 0 else (index + step) % size


def origin(index, step, size):
    return index ^ step if size & (size - 1) == 0 else (index - step) % size


def swap(value, axis, step):
    size = lax.axis_size(axis)
    return lax.ppermute(value, axis, [(i, mate(i, step, size)) for i in range(size)])


def limit(size):
    return pltpu.CompilerParams(vmem_limit_bytes=size)


def scores_kernel(table_ref, ids_ref, basis_ref, out_ref):
    samples = ids_ref.shape[0]
    rows = table_ref.shape[0]
    pick = ids_ref[...] == lax.broadcasted_iota(jnp.int32, (samples, rows), 1)
    chosen = jnp.dot(
        pick.astype(jnp.bfloat16), table_ref[...], preferred_element_type=jnp.float32
    ).astype(jnp.bfloat16)
    out_ref[...] = lax.dot_general(
        chosen, basis_ref[...], (((1,), (1,)), ((), ())), preferred_element_type=jnp.float32
    ).astype(jnp.bfloat16)


def partial_kernel(groups, per_group, tile, counts_ref, ids_ref, damage_ref, *refs):
    scores = refs[:groups]
    outs = refs[groups : 2 * groups]
    weight_ref, order_ref = refs[2 * groups :]
    me = lax.axis_index("grp")
    rows = scores[0].shape[1]
    slots = ids_ref.shape[1]
    total = lax.fori_loop(0, groups, lambda k, s: s + counts_ref[k], jnp.int32(0))
    live = lax.broadcasted_iota(jnp.int32, (1, slots), 1) < counts_ref[me]
    scale = jnp.where(live, 1.0 / total.astype(jnp.float32), 0.0)
    row = lax.broadcasted_iota(jnp.int32, (rows, slots), 0)
    weight = None
    for step in range(groups):
        first = origin(me, step, groups) * rows
        pick = (row + first == ids_ref[...]).astype(jnp.bfloat16)
        part = jnp.dot(scores[step][...], pick, preferred_element_type=jnp.float32)
        weight = part if weight is None else weight + part
    weight_ref[...] = jnp.where(live, weight * scale, 0.0).astype(jnp.bfloat16)
    for step in range(groups):
        first = pl.multiple_of(mate(me, step, groups) * per_group, per_group)
        order_ref[step * per_group : (step + 1) * per_group, :] = weight_ref[pl.ds(first, per_group), :]
    for start in range(0, damage_ref.shape[1], tile):
        part = jnp.dot(
            order_ref[...], damage_ref[:, start : start + tile], preferred_element_type=jnp.float32
        )
        for step in range(groups):
            block = part[step * per_group : (step + 1) * per_group, :]
            outs[step][:, start : start + tile] = block.astype(outs[step].dtype)


def values_kernel(own_ref, *refs):
    parts = refs[:-2]
    out_ref, stats_ref = refs[-2:]
    values = own_ref[...]
    for part in parts:
        values = values + part[...].astype(jnp.float32)
    out_ref[...] = values.astype(out_ref.dtype)
    rows = values.shape[0]
    square = jnp.sum(values * values, axis=1, keepdims=True)
    peak = jnp.max(values, axis=1, keepdims=True)
    stats_ref[0:1, :] = jnp.transpose(jnp.broadcast_to(square, (rows, 128)))[0:1, :]
    stats_ref[1:2, :] = jnp.transpose(jnp.broadcast_to(peak, (rows, 128)))[0:1, :]


def local(damage, basis_table, train_ids, counts, new_table, new_ids):
    slots, cells = damage.shape
    groups = lax.axis_size("grp")
    nodes = lax.axis_size("node")
    samples = new_ids.shape[0]
    per_group = samples // groups
    rows = basis_table.shape[0]

    scores = pl.pallas_call(
        scores_kernel,
        out_shape=jax.ShapeDtypeStruct((samples, rows), jnp.bfloat16),
        in_specs=[FULL, FULL, FULL],
        out_specs=FULL,
        compiler_params=limit(24 << 20),
        name="scores",
    )(new_table, new_ids.reshape(samples, 1), basis_table)

    every = [scores] + [swap(scores, "grp", step) for step in range(1, groups)]

    parts = pl.pallas_call(
        functools.partial(partial_kernel, groups, per_group, min(cells, 512)),
        out_shape=[
            jax.ShapeDtypeStruct((per_group, cells), jnp.float32 if step == 0 else jnp.bfloat16)
            for step in range(groups)
        ],
        in_specs=[SCALAR, FULL, FULL] + [FULL] * groups,
        out_specs=[FULL] * groups,
        scratch_shapes=[pltpu.VMEM((samples, slots), jnp.bfloat16)] * 2,
        compiler_params=limit(32 << 20),
        name="partial",
    )(counts, train_ids.reshape(1, slots), damage, *every)

    arrived = [swap(parts[step], "grp", step) for step in range(1, groups)]

    surrogate, stats = pl.pallas_call(
        values_kernel,
        out_shape=[
            jax.ShapeDtypeStruct((per_group, cells), jnp.bfloat16),
            jax.ShapeDtypeStruct((2, per_group), jnp.float32),
        ],
        in_specs=[FULL] * groups,
        out_specs=[FULL, FULL],
        compiler_params=limit(24 << 20),
        name="values",
    )(parts[0], *arrived)

    step = 1
    if nodes & (nodes - 1) == 0:
        while step < nodes:
            other = swap(stats, "node", step)
            stats = jnp.stack([stats[0] + other[0], jnp.maximum(stats[1], other[1])])
            step *= 2
        squares, peak = stats[0], stats[1]
    else:
        everything = lax.all_gather(stats, "node")
        squares, peak = jnp.sum(everything[:, 0], axis=0), jnp.max(everything[:, 1], axis=0)
    spread = jnp.sqrt(squares / (cells * nodes) + 1e-06)
    return (surrogate, peak, spread)


def solution(mesh):
    placed = (P("grp", "node"), P("grp", None), P("grp"), P(), P(), P())
    return jax.shard_map(
        local,
        mesh=mesh,
        in_specs=placed,
        out_specs=(P("grp", "node"), P("grp"), P("grp")),
        check_vma=False,
    )
```

```python
import functools

import jax
import jax.numpy as jnp
from jax import lax
from jax.experimental import pallas as pl
from jax.experimental.pallas import tpu as pltpu
from jax.sharding import PartitionSpec as P


FULL = pl.BlockSpec(memory_space=pltpu.VMEM)
FAR = pl.BlockSpec(memory_space=pltpu.HBM)


def mate(index, step, size):
    return index ^ step if size & (size - 1) == 0 else (index + step) % size


def origin(index, step, size):
    return index ^ step if size & (size - 1) == 0 else (index - step) % size


def swap(value, axis, step):
    size = lax.axis_size(axis)
    return lax.ppermute(value, axis, [(i, mate(i, step, size)) for i in range(size)])


def split_swap(value, steps):
    nodes = lax.axis_size("node")
    pairs = [
        (group * nodes + node, (group ^ steps[node % 2]) * nodes + node)
        for group in range(lax.axis_size("grp"))
        for node in range(nodes)
    ]
    return lax.ppermute(value, ("grp", "node"), pairs)


def params(size):
    return pltpu.CompilerParams(vmem_limit_bytes=size)


def cost(flops):
    return pl.CostEstimate(flops=flops, bytes_accessed=1 << 20, transcendentals=0)


def scores_kernel(groups, table_ref, ids_ref, basis_ref, train_ref, counts_ref, damage_ref, *refs):
    scores, half, named, damage, table, ids, basis, train, counts, choice, sems = refs
    pairs = (
        (counts_ref, counts),
        (ids_ref, ids),
        (train_ref, train),
        (table_ref, table),
        (basis_ref, basis),
        (damage_ref, damage),
    )
    copies = [pltpu.make_async_copy(src, dst, sems.at[k]) for k, (src, dst) in enumerate(pairs)]
    for copy in copies:
        copy.start()
    me = lax.axis_index("grp")
    samples = ids.shape[1]
    copies[1].wait()
    lane = lax.broadcasted_iota(jnp.int32, (samples, 128), 1)
    wanted = jnp.transpose(jnp.broadcast_to(ids[...].astype(jnp.float32), (128, samples)))
    for start in range(0, table.shape[0], 128):
        match = wanted == (lane + start).astype(jnp.float32)
        choice[:, start : start + 128] = match.astype(jnp.bfloat16)
    copies[0].wait()
    total = lax.fori_loop(0, groups, lambda k, s: s + counts[k], jnp.int32(0)).astype(jnp.float32)
    copies[3].wait()
    chosen = jnp.dot(choice[...], table[...], preferred_element_type=jnp.float32)
    copies[4].wait()
    found = lax.dot_general(
        chosen.astype(jnp.bfloat16),
        basis[...],
        (((1,), (1,)), ((), ())),
        preferred_element_type=jnp.float32,
    )
    scores[...] = (found / total).astype(jnp.bfloat16)
    rows = half.shape[0]
    odd = lax.axis_index("node") % 2
    half[...] = scores[pl.ds(pl.multiple_of(odd * rows, rows), rows), :]
    copies[2].wait()
    live = lax.broadcasted_iota(jnp.int32, named.shape, 1) < counts[me]
    named[...] = jnp.where(live, train[...], -1)
    copies[5].wait()


def picks_kernel(groups, named_ref, out_ref):
    me = lax.axis_index("grp")
    row = lax.broadcasted_iota(jnp.int32, out_ref.shape[1:], 0)
    for step in range(groups):
        first = origin(me, step, groups) * out_ref.shape[1]
        out_ref[step] = jnp.where(row == named_ref[...] - first, 1.0, 0.0).astype(out_ref.dtype)


def targets(paired, groups):
    if paired:
        odd = lax.axis_index("node") % 2
        return 3, [1 + odd], [2 - odd]
    return groups - 1, list(range(1, groups - 1)), []


def blocks(paired, groups, refs):
    if not paired:
        return [(refs[step], step) for step in range(groups)]
    own, near, mated, half, other, joined = refs
    odd = lax.axis_index("node") % 2
    rows = half.shape[0]
    joined[pl.ds(pl.multiple_of(odd * rows, rows), rows), :] = half[...]
    joined[pl.ds(pl.multiple_of((1 - odd) * rows, rows), rows), :] = other[...]
    return [(own, 0), (near, 1 + odd), (mated, 2 - odd), (joined, 3)]


def weights(groups, per_group, wanted, picks_ref, found, order_ref):
    me = lax.axis_index("grp")
    total = None
    for ref, step in found:
        for place, target in enumerate(wanted):
            first = pl.multiple_of(mate(me, target, groups) * per_group, per_group)
            order_ref[place * per_group : (place + 1) * per_group, :] = ref[pl.ds(first, per_group), :]
        part = jnp.dot(
            order_ref[: len(wanted) * per_group, :],
            picks_ref[step],
            preferred_element_type=jnp.float32,
        )
        total = part if total is None else total + part
    return total.astype(jnp.bfloat16)


def project(weight, damage_ref, outs, tile):
    rows = weight.shape[0] // len(outs)
    for start in range(0, damage_ref.shape[1], tile):
        part = jnp.dot(
            weight, damage_ref[:, start : start + tile], preferred_element_type=jnp.float32
        )
        for k, pieces in enumerate(outs):
            width = pieces[0].shape[1]
            out, at = pieces[start // width], start % width
            out[:, at : at + tile] = part[k * rows : (k + 1) * rows, :].astype(out.dtype)


def first_kernel(paired, groups, per_group, tile, picks_ref, damage_ref, *refs):
    refs, order = list(refs[:-1]), refs[-1]
    joined = [refs.pop()] if paired else []
    pieces = 2 if paired else 1
    scores, outs = refs[:-pieces], refs[-pieces:]
    first, _, _ = targets(paired, groups)
    found = blocks(paired, groups, scores + joined)
    weight = weights(groups, per_group, [first], picks_ref, found, order)
    project(weight, damage_ref, [outs], tile)


def other_kernel(paired, groups, per_group, tile, picks_ref, damage_ref, *refs):
    refs, order = list(refs[:-1]), refs[-1]
    joined = [refs.pop()] if paired else []
    _, sent, kept = targets(paired, groups)
    count = len(sent) + 2 * len(kept)
    scores, outs, own = refs[: -count - 1], refs[-count - 1 : -1], refs[-1]
    found = blocks(paired, groups, scores + joined)
    weight = weights(groups, per_group, sent + kept + [0], picks_ref, found, order)
    rows = (len(sent) + len(kept)) * per_group
    own[...] = weight[rows:, :]
    outs = [[out] for out in outs[: len(sent)]] + ([outs[len(sent) :]] if kept else [])
    project(weight[:rows, :], damage_ref, outs, tile)


def own_kernel(tile, weight_ref, damage_ref, out_ref):
    project(weight_ref[...], damage_ref, [[out_ref]], tile)


def add_kernel(one_ref, two_ref, out_ref):
    out_ref[...] = (one_ref[...] + two_ref[...].astype(jnp.float32)).astype(out_ref.dtype)


def values_kernel(own_ref, *refs):
    parts, (out_ref, stats_ref) = refs[:-2], refs[-2:]
    rows, cells = out_ref.shape
    square = peak = None
    width = min(part.shape[1] for part in parts)
    for start in range(0, cells, width):
        values = own_ref[:, start : start + width]
        place = 0
        for part in parts:
            if place <= start < place + part.shape[1]:
                values = values + part[:, start - place : start - place + width].astype(jnp.float32)
            place = (place + part.shape[1]) % cells
        out_ref[:, start : start + width] = values
        more = jnp.sum(values * values, axis=1, keepdims=True)
        high = jnp.max(values, axis=1, keepdims=True)
        square = more if square is None else square + more
        peak = high if peak is None else jnp.maximum(peak, high)
    stats_ref[0:1, :] = jnp.transpose(jnp.broadcast_to(square, (rows, 128)))[0:1, :]
    stats_ref[1:2, :] = jnp.transpose(jnp.broadcast_to(peak, (rows, 128)))[0:1, :]


def round_kernel(values_ref, out_ref):
    out_ref[...] = values_ref[...].astype(out_ref.dtype)


def combine(first, second):
    return jnp.stack([first[0] + second[0], jnp.maximum(first[1], second[1])])


def over_nodes(stats, nodes):
    if nodes & (nodes - 1):
        everything = lax.all_gather(stats, "node")
        return jnp.stack([jnp.sum(everything[:, 0], axis=0), jnp.max(everything[:, 1], axis=0)])
    step = 1
    while step < nodes:
        stats = combine(stats, swap(stats, "node", step))
        step *= 2
    return stats


def local(damage, basis_table, train_ids, counts, new_table, new_ids):
    slots, cells = damage.shape
    groups = lax.axis_size("grp")
    nodes = lax.axis_size("node")
    samples = new_ids.shape[0]
    per_group = samples // groups
    rows = basis_table.shape[0]
    half = jnp.bfloat16
    paired = groups == 4 and nodes % 2 == 0

    far = [
        pltpu.with_memory_space_constraint(x, pltpu.HBM)
        for x in (
            new_table,
            new_ids.reshape(1, samples),
            basis_table,
            train_ids.reshape(1, slots),
            counts,
            damage,
        )
    ]
    scores, own_half, named, damage = pl.pallas_call(
        functools.partial(scores_kernel, groups),
        out_shape=[
            jax.ShapeDtypeStruct((samples, rows), half),
            jax.ShapeDtypeStruct((samples // 2, rows), half),
            jax.ShapeDtypeStruct((1, slots), jnp.int32),
            jax.ShapeDtypeStruct((slots, cells), half),
        ],
        in_specs=[FAR] * 6,
        out_specs=[FULL] * 4,
        scratch_shapes=[
            pltpu.VMEM(new_table.shape, half),
            pltpu.VMEM((1, samples), jnp.int32),
            pltpu.VMEM(basis_table.shape, half),
            pltpu.VMEM((1, slots), jnp.int32),
            pltpu.SMEM((groups,), jnp.int32),
            pltpu.VMEM((samples, new_table.shape[0]), half),
            pltpu.SemaphoreType.DMA((6,)),
        ],
        compiler_params=params(32 << 20),
        name="scores",
    )(*far)

    picks = pl.pallas_call(
        functools.partial(picks_kernel, groups),
        out_shape=jax.ShapeDtypeStruct((groups, rows, slots), half),
        in_specs=[FULL],
        out_specs=FULL,
        compiler_params=params(16 << 20),
        cost_estimate=cost(1 << 20),
        name="picks",
    )(named)

    if paired:
        opposite = swap(own_half, "grp", 3)
        near = split_swap(scores, (1, 2))
        every = [scores, near, swap(near, "node", 1), opposite, swap(opposite, "node", 1)]
        width = cells // 2
        kinds = [(cells, half)] + [(width, jnp.float32)] * 2
        joined = [pltpu.VMEM((samples, rows), half)]
    else:
        every = [scores] + [swap(scores, "grp", step) for step in range(1, groups)]
        width = cells
        kinds = [(cells, half)] * (groups - 2)
        joined = []
    tile = min(width, 512)

    first = pl.pallas_call(
        functools.partial(first_kernel, paired, groups, per_group, tile),
        out_shape=[jax.ShapeDtypeStruct((per_group, width), half)] * (cells // width),
        in_specs=[FULL] * (2 + len(every)),
        out_specs=[FULL] * (cells // width),
        scratch_shapes=joined + [pltpu.VMEM((per_group, rows), half)],
        compiler_params=params(24 << 20),
        cost_estimate=cost(1 << 20),
        name="first",
    )(picks, damage, *every)
    if paired:
        passed = [split_swap(part, (1, 2)) for part in first]
    else:
        arrived = [swap(first[0], "grp", groups - 1)]

    wanted = 3 if paired else groups - 1
    *made, own_weight = pl.pallas_call(
        functools.partial(other_kernel, paired, groups, per_group, tile),
        out_shape=[jax.ShapeDtypeStruct((per_group, size), kind) for size, kind in kinds]
        + [jax.ShapeDtypeStruct((per_group, slots), half)],
        in_specs=[FULL] * (2 + len(every)),
        out_specs=[FULL] * (len(kinds) + 1),
        scratch_shapes=joined + [pltpu.VMEM((wanted * per_group, rows), half)],
        compiler_params=params(32 << 20),
        cost_estimate=cost(1 << 20),
        name="other",
    )(picks, damage, *every)
    if paired:
        add = pl.pallas_call(
            add_kernel,
            out_shape=jax.ShapeDtypeStruct((per_group, width), half),
            in_specs=[FULL] * 2,
            out_specs=FULL,
            compiler_params=params(16 << 20),
            cost_estimate=cost(1 << 20),
            name="add",
        )
        arrived = [split_swap(made[0], (1, 2))] + [
            split_swap(add(made[1 + k], passed[k]), (2, 1)) for k in range(2)
        ]
    else:
        arrived += [swap(part, "grp", step) for step, part in enumerate(made, 1)]

    own = pl.pallas_call(
        functools.partial(own_kernel, tile),
        out_shape=jax.ShapeDtypeStruct((per_group, cells), jnp.float32),
        in_specs=[FULL, FULL],
        out_specs=FULL,
        compiler_params=params(24 << 20),
        cost_estimate=cost(1 << 20),
        name="own",
    )(own_weight, damage)

    values, stats = pl.pallas_call(
        values_kernel,
        out_shape=[
            jax.ShapeDtypeStruct((per_group, cells), jnp.float32),
            jax.ShapeDtypeStruct((2, per_group), jnp.float32),
        ],
        in_specs=[FULL] * (1 + len(arrived)),
        out_specs=[FULL, FULL],
        compiler_params=params(24 << 20),
        name="values",
    )(own, *arrived)
    surrogate = pl.pallas_call(
        round_kernel,
        out_shape=jax.ShapeDtypeStruct((per_group, cells), half),
        in_specs=[FULL],
        out_specs=FULL,
        compiler_params=params(16 << 20),
        cost_estimate=cost(1 << 20),
        name="round",
    )(values)

    squares, peak = over_nodes(stats, nodes)
    spread = jnp.sqrt(squares / (cells * nodes) + 1e-06)
    return (surrogate, peak, spread)


def solution(mesh):
    placed = (P("grp", "node"), P("grp", None), P("grp"), P(), P(), P())
    return jax.shard_map(
        local,
        mesh=mesh,
        in_specs=placed,
        out_specs=(P("grp", "node"), P("grp"), P("grp")),
        check_vma=False,
    )
```

```python
import functools

import jax
import jax.numpy as jnp
from jax import lax
from jax.experimental import pallas as pl
from jax.experimental.pallas import tpu as pltpu
from jax.sharding import PartitionSpec as P


FULL = pl.BlockSpec(memory_space=pltpu.VMEM)
FAR = pl.BlockSpec(memory_space=pltpu.HBM)


def mate(index, step, size):
    return index ^ step if size & (size - 1) == 0 else (index + step) % size


def origin(index, step, size):
    return index ^ step if size & (size - 1) == 0 else (index - step) % size


def swap(value, axis, step):
    size = lax.axis_size(axis)
    return lax.ppermute(value, axis, [(i, mate(i, step, size)) for i in range(size)])


def split_swap(value, steps):
    nodes = lax.axis_size("node")
    pairs = [
        (group * nodes + node, (group ^ steps[node % 2]) * nodes + node)
        for group in range(lax.axis_size("grp"))
        for node in range(nodes)
    ]
    return lax.ppermute(value, ("grp", "node"), pairs)


def scores_kernel(groups, table_ref, ids_ref, basis_ref, train_ref, counts_ref, damage_ref, *refs):
    (scores, named, damage), sends = refs[:3], refs[3:-7]
    table, ids, basis, train, counts, choice, sems = refs[-7:]
    pairs = (
        (ids_ref, ids),
        (table_ref, table),
        (basis_ref, basis),
        (counts_ref, counts),
        (train_ref, train),
        (damage_ref, damage),
    )
    copies = [pltpu.make_async_copy(src, dst, sems.at[k]) for k, (src, dst) in enumerate(pairs)]
    for copy in copies:
        copy.start()
    me = lax.axis_index("grp")
    samples = ids.shape[1]
    copies[0].wait()
    lane = lax.broadcasted_iota(jnp.int32, (samples, 128), 1)
    wanted = jnp.transpose(jnp.broadcast_to(ids[...].astype(jnp.float32), (128, samples)))
    for start in range(0, table.shape[0], 128):
        match = wanted == (lane + start).astype(jnp.float32)
        choice[:, start : start + 128] = match.astype(jnp.bfloat16)
    copies[1].wait()
    chosen = jnp.dot(choice[...], table[...], preferred_element_type=jnp.float32)
    copies[2].wait()
    found = lax.dot_general(
        chosen.astype(jnp.bfloat16),
        basis[...],
        (((1,), (1,)), ((), ())),
        preferred_element_type=jnp.float32,
    )
    copies[3].wait()
    total = lax.fori_loop(0, groups, lambda k, s: s + counts[k], jnp.int32(0)).astype(jnp.float32)
    scores[...] = (found / total).astype(jnp.bfloat16)
    if sends:
        odd = lax.axis_index("node") % 2
        near_head, near_tail, side_head, side_tail = sends
        per_group = near_head.shape[0]
        other = me ^ (1 + 2 * odd)
        near_head[...] = rows_of(scores, other ^ 3, per_group)
        for place, step in enumerate((1, 2, 0)):
            near_tail[place * per_group : (place + 1) * per_group, :] = rows_of(
                scores, other ^ step, per_group
            )
        small = per_group // 2
        side_head[...] = rows_of(scores, (me ^ 1) * 2 + odd, small)
        for place in range(3):
            piece = odd * 3 + place
            step = jnp.where(piece // 2 == 0, 1, jnp.where(piece // 2 == 1, 2, 0))
            side_tail[place * small : (place + 1) * small, :] = rows_of(
                scores, (me ^ 2 ^ step) * 2 + piece % 2, small
            )
    copies[4].wait()
    live = lax.broadcasted_iota(jnp.int32, named.shape, 1) < counts[me]
    named[...] = jnp.where(live, train[...], -1)
    copies[5].wait()


def rows_of(ref, block, rows):
    return ref[pl.ds(pl.multiple_of(block * rows, rows), rows), :]


def picks_kernel(groups, named_ref, out_ref):
    me = lax.axis_index("grp")
    row = lax.broadcasted_iota(jnp.int32, out_ref.shape[1:], 0)
    for step in range(groups):
        first = origin(me, step, groups) * out_ref.shape[1]
        out_ref[step] = jnp.where(row == named_ref[...] - first, 1.0, 0.0).astype(out_ref.dtype)


def join(half_ref, other_ref, joined):
    odd = lax.axis_index("node") % 2
    rows = half_ref.shape[0]
    joined[pl.ds(pl.multiple_of(odd * rows, rows), rows), :] = half_ref[...]
    joined[pl.ds(pl.multiple_of((1 - odd) * rows, rows), rows), :] = other_ref[...]


def project(weight, damage_ref, start, outs, tile):
    rows = weight.shape[0] // len(outs)
    for at in range(0, outs[0].shape[1], tile):
        part = jnp.dot(
            weight,
            damage_ref[:, start + at : start + at + tile],
            preferred_element_type=jnp.float32,
        )
        for k, out in enumerate(outs):
            out[:, at : at + tile] = part[k * rows : (k + 1) * rows, :].astype(out.dtype)


def first_kernel(tile, picks_ref, damage_ref, own, near, mated, half, other, weight, out, joined):
    odd = lax.axis_index("node") % 2
    join(half, other, joined)
    total = jnp.dot(
        rows_of(own, lax.axis_index("grp") ^ 3, near.shape[0]),
        picks_ref[0],
        preferred_element_type=jnp.float32,
    )
    for ref, step in ((near, 1 + 2 * odd), (mated, 3 - 2 * odd), (joined, 2)):
        total += jnp.dot(ref[...], picks_ref[step], preferred_element_type=jnp.float32)
    weight[...] = total.astype(weight.dtype)
    project(weight[...], damage_ref, 0, [out], tile)


def second_kernel(tile, weight_ref, damage_ref, out_ref):
    project(weight_ref[...], damage_ref, damage_ref.shape[1] - out_ref.shape[1], [out_ref], tile)


def other_kernel(tile, picks_ref, damage_ref, own, near, mated, half, other, *refs):
    sent, kept, later, weight, order, joined = refs
    odd = lax.axis_index("node") % 2
    me = lax.axis_index("grp")
    join(half, other, joined)
    rows = sent.shape[0]
    steps = (1 + odd, 2 - odd, 0)
    total = None
    for ref, step in ((own, 0), (near, 1 + 2 * odd), (mated, 3 - 2 * odd), (joined, 2)):
        for place, target in enumerate(steps):
            block = me ^ target if ref is own else (odd, 1 - odd, 2)[place]
            order[place * rows : (place + 1) * rows, :] = rows_of(ref, block, rows)
        part = jnp.dot(order[...], picks_ref[step], preferred_element_type=jnp.float32)
        total = part if total is None else total + part
    total = total.astype(jnp.bfloat16)
    weight[...] = total[2 * rows :, :]
    width = kept.shape[1]
    for start, keep in ((0, kept), (width, later)):
        for at in range(0, width, tile):
            part = jnp.dot(
                total[: 2 * rows, :],
                damage_ref[:, start + at : start + at + tile],
                preferred_element_type=jnp.float32,
            )
            sent[:, start + at : start + at + tile] = part[:rows, :].astype(sent.dtype)
            keep[:, at : at + tile] = part[rows:, :]


def direct_kernel(groups, tile, picks_ref, damage_ref, *refs):
    scores, outs, order = refs[:groups], refs[groups:-1], refs[-1]
    me = lax.axis_index("grp")
    rows = outs[0].shape[0]
    total = None
    for step in range(groups):
        for target in range(groups):
            order[target * rows : (target + 1) * rows, :] = rows_of(
                scores[step], mate(me, target, groups), rows
            )
        part = jnp.dot(order[...], picks_ref[step], preferred_element_type=jnp.float32)
        total = part if total is None else total + part
    project(total.astype(jnp.bfloat16), damage_ref, 0, outs, tile)


def own_kernel(tile, weight_ref, damage_ref, out_ref):
    project(weight_ref[...], damage_ref, 0, [out_ref], tile)


def add_kernel(one_ref, two_ref, out_ref):
    out_ref[...] = (one_ref[...] + two_ref[...].astype(jnp.float32)).astype(out_ref.dtype)


def values_kernel(own_ref, *refs):
    parts, (out_ref, stats_ref) = refs[:-2], refs[-2:]
    rows, cells = out_ref.shape
    square = peak = None
    width = min(part.shape[1] for part in parts)
    for start in range(0, cells, width):
        values = own_ref[:, start : start + width]
        place = 0
        for part in parts:
            if place <= start < place + part.shape[1]:
                values = values + part[:, start - place : start - place + width].astype(jnp.float32)
            place = (place + part.shape[1]) % cells
        out_ref[:, start : start + width] = values
        more = jnp.sum(values * values, axis=1, keepdims=True)
        high = jnp.max(values, axis=1, keepdims=True)
        square = more if square is None else square + more
        peak = high if peak is None else jnp.maximum(peak, high)
    stats_ref[0:1, :] = jnp.transpose(jnp.broadcast_to(square, (rows, 128)))[0:1, :]
    stats_ref[1:2, :] = jnp.transpose(jnp.broadcast_to(peak, (rows, 128)))[0:1, :]


def round_kernel(values_ref, out_ref):
    out_ref[...] = values_ref[...].astype(out_ref.dtype)


def combine(first, second):
    return jnp.stack([first[0] + second[0], jnp.maximum(first[1], second[1])])


def over_nodes(stats, nodes):
    if nodes & (nodes - 1):
        everything = lax.all_gather(stats, "node")
        return jnp.stack([jnp.sum(everything[:, 0], axis=0), jnp.max(everything[:, 1], axis=0)])
    step = 1
    while step < nodes:
        stats = combine(stats, swap(stats, "node", step))
        step *= 2
    return stats


def call(kernel, outs, ins, *args, scratch=(), limit=24):
    return pl.pallas_call(
        kernel,
        out_shape=[jax.ShapeDtypeStruct(shape, kind) for shape, kind in outs],
        in_specs=ins,
        out_specs=[FULL] * len(outs),
        scratch_shapes=list(scratch),
        compiler_params=pltpu.CompilerParams(vmem_limit_bytes=limit << 20),
        cost_estimate=pl.CostEstimate(flops=1 << 20, bytes_accessed=1 << 20, transcendentals=0),
    )(*args)


def local(damage, basis_table, train_ids, counts, new_table, new_ids):
    slots, cells = damage.shape
    groups = lax.axis_size("grp")
    nodes = lax.axis_size("node")
    samples = new_ids.shape[0]
    per_group = samples // groups
    rows = basis_table.shape[0]
    half, full = jnp.bfloat16, jnp.float32
    paired = is_paired(groups, nodes)
    operands = (new_table, new_ids.reshape(1, samples), basis_table, train_ids.reshape(1, slots), counts, damage)
    rest = samples - per_group
    sends = [(per_group, rows), (rest, rows), (per_group // 2, rows), (rest // 2, rows)]
    scores, named, damage, *sends = call(
        functools.partial(scores_kernel, groups),
        [((samples, rows), half), ((1, slots), jnp.int32), ((slots, cells), half)]
        + ([(shape, half) for shape in sends] if paired else []),
        [FAR] * 6,
        *[pltpu.with_memory_space_constraint(x, pltpu.HBM) for x in operands],
        scratch=[
            pltpu.VMEM(new_table.shape, half),
            pltpu.VMEM((1, samples), jnp.int32),
            pltpu.VMEM(basis_table.shape, half),
            pltpu.VMEM((1, slots), jnp.int32),
            pltpu.SMEM((groups,), jnp.int32),
            pltpu.VMEM((samples, new_table.shape[0]), half),
            pltpu.SemaphoreType.DMA((6,)),
        ],
        limit=32,
    )
    picks = call(
        functools.partial(picks_kernel, groups), [((groups, rows, slots), half)], [FULL], named
    )[0]
    part = ((per_group, cells), half)

    if paired:
        width = cells // 2
        tile = min(width, 512)
        piece = (per_group, width)
        near_head, near_tail, side_head, side_tail = sends
        side_head = swap(side_head, "grp", 2)
        near_head = split_swap(near_head, (1, 3))
        side_tail = swap(side_tail, "grp", 2)
        near_tail = split_swap(near_tail, (1, 3))
        heads = (near_head, swap(near_head, "node", 1), side_head, swap(side_head, "node", 1))
        tails = (near_tail, swap(near_tail, "node", 1), side_tail, swap(side_tail, "node", 1))
        weight, first = call(
            functools.partial(first_kernel, tile),
            [((per_group, slots), half), (piece, half)],
            [FULL] * 7,
            picks,
            damage,
            scores,
            *heads,
            scratch=[pltpu.VMEM((per_group, rows), half)],
        )
        second = call(
            functools.partial(second_kernel, tile), [(piece, half)], [FULL] * 2, weight, damage
        )[0]
        passed = [split_swap(x, (1, 2)) for x in (first, second)]
        sent, *kept, weight = call(
            functools.partial(other_kernel, tile),
            [part, (piece, full), (piece, full), ((per_group, slots), half)],
            [FULL] * 7,
            picks,
            damage,
            scores,
            *tails,
            scratch=[pltpu.VMEM((rest, rows), half)] * 2,
        )
        arrived = [split_swap(sent, (1, 2))]
        for k in range(2):
            both = call(add_kernel, [(piece, half)], [FULL] * 2, kept[k], passed[k])[0]
            arrived.append(split_swap(both, (2, 1)))
        own = call(
            functools.partial(own_kernel, tile), [((per_group, cells), full)], [FULL] * 2, weight, damage
        )[0]
    else:
        every = [scores] + [swap(scores, "grp", step) for step in range(1, groups)]
        own, *parts = call(
            functools.partial(direct_kernel, groups, min(cells, 512)),
            [((per_group, cells), full)] + [part] * (groups - 1),
            [FULL] * (2 + groups),
            picks,
            damage,
            *every,
            scratch=[pltpu.VMEM((samples, rows), half)],
            limit=32,
        )
        arrived = [swap(x, "grp", step) for step, x in enumerate(parts, 1)]

    values, stats = call(
        values_kernel,
        [((per_group, cells), full), ((2, per_group), full)],
        [FULL] * (1 + len(arrived)),
        own,
        *arrived,
    )
    surrogate = call(round_kernel, [part], [FULL], values)[0]
    squares, peak = over_nodes(stats, nodes)
    spread = jnp.sqrt(squares / (cells * nodes) + 1e-06)
    return (surrogate, peak, spread)


def is_paired(groups, nodes):
    return groups == 4 and nodes % 2 == 0


def solution(mesh):
    placed = (P("grp", "node"), P("grp", None), P("grp"), P(), P(), P())
    return jax.shard_map(
        local,
        mesh=mesh,
        in_specs=placed,
        out_specs=(P("grp", "node"), P("grp"), P("grp")),
        check_vma=False,
    )
```

```python
import functools
import math

import jax
import jax.numpy as jnp
from jax import lax
from jax.experimental import pallas as pl
from jax.experimental.pallas import tpu as pltpu
from jax.sharding import PartitionSpec as P


FULL = pl.BlockSpec(memory_space=pltpu.VMEM)
FAR = pl.BlockSpec(memory_space=pltpu.HBM)


def mate(index, step, size):
    return index ^ step if size & (size - 1) == 0 else (index + step) % size


def origin(index, step, size):
    return index ^ step if size & (size - 1) == 0 else (index - step) % size


def swap(value, axis, step):
    size = lax.axis_size(axis)
    return lax.ppermute(value, axis, [(i, mate(i, step, size)) for i in range(size)])


def split_swap(value, steps):
    nodes = lax.axis_size("node")
    pairs = [
        (group * nodes + node, (group ^ steps[node % 2]) * nodes + node)
        for group in range(lax.axis_size("grp"))
        for node in range(nodes)
    ]
    return lax.ppermute(value, ("grp", "node"), pairs)


def node_swap(value, steps):
    pairs = [(node, node ^ steps[node % 2]) for node in range(lax.axis_size("node"))]
    return lax.ppermute(value, "node", pairs)


def scores_kernel(groups, table_ref, ids_ref, basis_ref, train_ref, counts_ref, damage_ref, *refs):
    (scores, named, damage), sends = refs[:3], refs[3:-7]
    table, ids, basis, train, counts, choice, sems = refs[-7:]
    pairs = (
        (ids_ref, ids),
        (table_ref, table),
        (basis_ref, basis),
        (counts_ref, counts),
        (train_ref, train),
        (damage_ref, damage),
    )
    copies = [pltpu.make_async_copy(src, dst, sems.at[k]) for k, (src, dst) in enumerate(pairs)]
    for copy in copies:
        copy.start()
    me = lax.axis_index("grp")
    samples = ids.shape[1]
    copies[0].wait()
    lane = lax.broadcasted_iota(jnp.int32, (samples, 128), 1)
    wanted = jnp.transpose(jnp.broadcast_to(ids[...].astype(jnp.float32), (128, samples)))
    for start in range(0, table.shape[0], 128):
        match = wanted == (lane + start).astype(jnp.float32)
        choice[:, start : start + 128] = match.astype(jnp.bfloat16)
    copies[1].wait()
    chosen = jnp.dot(choice[...], table[...], preferred_element_type=jnp.float32)
    copies[2].wait()
    found = lax.dot_general(
        chosen.astype(jnp.bfloat16),
        basis[...],
        (((1,), (1,)), ((), ())),
        preferred_element_type=jnp.float32,
    )
    copies[3].wait()
    total = lax.fori_loop(0, groups, lambda k, s: s + counts[k], jnp.int32(0)).astype(jnp.float32)
    scores[...] = (found * (1.0 / total)).astype(jnp.bfloat16)
    if sends:
        odd = lax.axis_index("node") % 2
        near_head, near_tail, side_head, side_tail = sends
        per_group = near_head.shape[0]
        other = me ^ (1 + 2 * odd)
        near_head[...] = rows_of(scores, other ^ 3, per_group)
        for place, step in enumerate((1, 2, 0)):
            near_tail[place * per_group : (place + 1) * per_group, :] = rows_of(
                scores, other ^ step, per_group
            )
        small = per_group // 2
        side_head[...] = rows_of(scores, (me ^ 1) * 2 + odd, small)
        for place in range(3):
            piece = odd * 3 + place
            step = jnp.where(piece // 2 == 0, 1, jnp.where(piece // 2 == 1, 2, 0))
            side_tail[place * small : (place + 1) * small, :] = rows_of(
                scores, (me ^ 2 ^ step) * 2 + piece % 2, small
            )
    copies[4].wait()
    live = lax.broadcasted_iota(jnp.int32, named.shape, 1) < counts[me]
    named[...] = jnp.where(live, train[...], -1)
    copies[5].wait()


def rows_of(ref, block, rows):
    return ref[pl.ds(pl.multiple_of(block * rows, rows), rows), :]


def picks_kernel(groups, named_ref, out_ref):
    me = lax.axis_index("grp")
    row = lax.broadcasted_iota(jnp.int32, out_ref.shape[1:], 0)
    for step in range(groups):
        first = origin(me, step, groups) * out_ref.shape[1]
        out_ref[step] = jnp.where(row == named_ref[...] - first, 1.0, 0.0).astype(out_ref.dtype)


def join(half_ref, other_ref, joined):
    odd = lax.axis_index("node") % 2
    rows = half_ref.shape[0]
    joined[pl.ds(pl.multiple_of(odd * rows, rows), rows), :] = half_ref[...]
    joined[pl.ds(pl.multiple_of((1 - odd) * rows, rows), rows), :] = other_ref[...]


def project(weight, damage_ref, start, outs, tile):
    rows = weight.shape[0] // len(outs)
    for at in range(0, outs[0].shape[1], tile):
        part = jnp.dot(
            weight,
            damage_ref[:, start + at : start + at + tile],
            preferred_element_type=jnp.float32,
        )
        for k, out in enumerate(outs):
            out[:, at : at + tile] = part[k * rows : (k + 1) * rows, :].astype(out.dtype)


def first_kernel(tile, picks_ref, damage_ref, own, near, mated, half, other, weight, out, joined):
    odd = lax.axis_index("node") % 2
    join(half, other, joined)
    total = jnp.dot(
        rows_of(own, lax.axis_index("grp") ^ 3, near.shape[0]),
        picks_ref[0],
        preferred_element_type=jnp.float32,
    )
    for ref, step in ((near, 1 + 2 * odd), (mated, 3 - 2 * odd), (joined, 2)):
        total += jnp.dot(ref[...], picks_ref[step], preferred_element_type=jnp.float32)
    weight[...] = total.astype(weight.dtype)
    project(weight[...], damage_ref, 0, [out], tile)


def second_kernel(tile, weight_ref, damage_ref, out_ref):
    project(weight_ref[...], damage_ref, damage_ref.shape[1] - out_ref.shape[1], [out_ref], tile)


def other_kernel(tile, picks_ref, damage_ref, own, near, mated, half, other, *refs):
    sent, kept, later, weight, order, joined = refs
    odd = lax.axis_index("node") % 2
    me = lax.axis_index("grp")
    join(half, other, joined)
    rows = sent.shape[0]
    steps = (1 + odd, 2 - odd, 0)
    total = None
    for ref, step in ((own, 0), (near, 1 + 2 * odd), (mated, 3 - 2 * odd), (joined, 2)):
        for place, target in enumerate(steps):
            block = me ^ target if ref is own else (odd, 1 - odd, 2)[place]
            order[place * rows : (place + 1) * rows, :] = rows_of(ref, block, rows)
        part = jnp.dot(order[...], picks_ref[step], preferred_element_type=jnp.float32)
        total = part if total is None else total + part
    total = total.astype(jnp.bfloat16)
    weight[...] = total[2 * rows :, :]
    for start, keep in ((0, kept), (kept.shape[1], later)):
        for at in range(0, keep.shape[1], tile):
            part = jnp.dot(
                total[: 2 * rows, :],
                damage_ref[:, start + at : start + at + tile],
                preferred_element_type=jnp.float32,
            )
            sent[:, start + at : start + at + tile] = part[:rows, :].astype(sent.dtype)
            keep[:, at : at + tile] = part[rows:, :]


def direct_kernel(groups, tile, picks_ref, damage_ref, *refs):
    scores, outs, order = refs[:groups], refs[groups:-1], refs[-1]
    me = lax.axis_index("grp")
    rows = outs[0].shape[0]
    total = None
    for step in range(groups):
        for target in range(groups):
            order[target * rows : (target + 1) * rows, :] = rows_of(
                scores[step], mate(me, target, groups), rows
            )
        part = jnp.dot(order[...], picks_ref[step], preferred_element_type=jnp.float32)
        total = part if total is None else total + part
    project(total.astype(jnp.bfloat16), damage_ref, 0, outs, tile)


def own_kernel(tile, weight_ref, damage_ref, out_ref):
    project(weight_ref[...], damage_ref, 0, [out_ref], tile)


def add_kernel(one_ref, two_ref, out_ref):
    out_ref[...] = (one_ref[...] + two_ref[...].astype(jnp.float32)).astype(out_ref.dtype)


def values_kernel(own_ref, *refs):
    parts, (out_ref, stats_ref) = refs[:-2], refs[-2:]
    rows, cells = out_ref.shape
    square = peak = None
    width = math.gcd(512, *[part.shape[1] for part in parts])
    for start in range(0, cells, width):
        values = own_ref[:, start : start + width]
        place = 0
        for part in parts:
            if place <= start < place + part.shape[1]:
                values = values + part[:, start - place : start - place + width].astype(jnp.float32)
            place = (place + part.shape[1]) % cells
        out_ref[:, start : start + width] = values
        more = jnp.sum(values * values, axis=1, keepdims=True)
        high = jnp.max(values, axis=1, keepdims=True)
        square = more if square is None else square + more
        peak = high if peak is None else jnp.maximum(peak, high)
    stats_ref[0:1, :] = jnp.transpose(jnp.broadcast_to(square, (rows, 128)))[0:1, :]
    stats_ref[1:2, :] = jnp.transpose(jnp.broadcast_to(peak, (rows, 128)))[0:1, :]


def round_kernel(values_ref, out_ref):
    out_ref[...] = values_ref[...].astype(out_ref.dtype)


def combine(first, second):
    return jnp.stack([first[0] + second[0], jnp.maximum(first[1], second[1])])


def over_nodes(stats, nodes):
    if nodes & (nodes - 1):
        everything = lax.all_gather(stats, "node")
        return jnp.stack([jnp.sum(everything[:, 0], axis=0), jnp.max(everything[:, 1], axis=0)])
    if nodes == 8:
        pair = combine(stats, node_swap(stats, (1, 1)))
        across = node_swap(pair, (4, 6))
        beside = node_swap(pair, (2, 2))
        return combine(combine(pair, beside), combine(across, node_swap(across, (1, 1))))
    step = 1
    while step < nodes:
        stats = combine(stats, swap(stats, "node", step))
        step *= 2
    return stats


def call(kernel, outs, ins, *args, scratch=(), limit=24):
    return pl.pallas_call(
        kernel,
        out_shape=[jax.ShapeDtypeStruct(shape, kind) for shape, kind in outs],
        in_specs=ins,
        out_specs=[FULL] * len(outs),
        scratch_shapes=list(scratch),
        compiler_params=pltpu.CompilerParams(vmem_limit_bytes=limit << 20),
        cost_estimate=pl.CostEstimate(flops=1 << 20, bytes_accessed=1 << 20, transcendentals=0),
    )(*args)


def local(damage, basis_table, train_ids, counts, new_table, new_ids):
    slots, cells = damage.shape
    groups = lax.axis_size("grp")
    nodes = lax.axis_size("node")
    samples = new_ids.shape[0]
    per_group = samples // groups
    rows = basis_table.shape[0]
    half, full = jnp.bfloat16, jnp.float32
    paired = is_paired(groups, nodes)
    operands = (new_table, new_ids.reshape(1, samples), basis_table, train_ids.reshape(1, slots), counts, damage)
    rest = samples - per_group
    sends = [(per_group, rows), (rest, rows), (per_group // 2, rows), (rest // 2, rows)]
    scores, named, damage, *sends = call(
        functools.partial(scores_kernel, groups),
        [((samples, rows), half), ((1, slots), jnp.int32), ((slots, cells), half)]
        + ([(shape, half) for shape in sends] if paired else []),
        [FAR] * 6,
        *[pltpu.with_memory_space_constraint(x, pltpu.HBM) for x in operands],
        scratch=[
            pltpu.VMEM(new_table.shape, half),
            pltpu.VMEM((1, samples), jnp.int32),
            pltpu.VMEM(basis_table.shape, half),
            pltpu.VMEM((1, slots), jnp.int32),
            pltpu.SMEM((groups,), jnp.int32),
            pltpu.VMEM((samples, new_table.shape[0]), half),
            pltpu.SemaphoreType.DMA((6,)),
        ],
        limit=32,
    )
    picks = call(
        functools.partial(picks_kernel, groups), [((groups, rows, slots), half)], [FULL], named
    )[0]
    part = ((per_group, cells), half)

    if paired:
        widths = split_columns(cells)
        tile = math.gcd(512, *widths)
        pieces = [(per_group, width) for width in widths]
        near_head, near_tail, side_head, side_tail = sends
        side_head = swap(side_head, "grp", 2)
        near_head = split_swap(near_head, (1, 3))
        side_tail = swap(side_tail, "grp", 2)
        near_tail = split_swap(near_tail, (1, 3))
        heads = (near_head, swap(near_head, "node", 1), side_head, swap(side_head, "node", 1))
        tails = (near_tail, swap(near_tail, "node", 1), side_tail, swap(side_tail, "node", 1))
        weight, first = call(
            functools.partial(first_kernel, tile),
            [((per_group, slots), half), (pieces[0], half)],
            [FULL] * 7,
            picks,
            damage,
            scores,
            *heads,
            scratch=[pltpu.VMEM((per_group, rows), half)],
        )
        second = call(
            functools.partial(second_kernel, tile), [(pieces[1], half)], [FULL] * 2, weight, damage
        )[0]
        passed = [split_swap(x, (1, 2)) for x in (first, second)]
        sent, *kept, weight = call(
            functools.partial(other_kernel, tile),
            [part, (pieces[0], full), (pieces[1], full), ((per_group, slots), half)],
            [FULL] * 7,
            picks,
            damage,
            scores,
            *tails,
            scratch=[pltpu.VMEM((rest, rows), half)] * 2,
        )
        arrived = [split_swap(sent, (1, 2))]
        for k in range(2):
            both = call(add_kernel, [(pieces[k], half)], [FULL] * 2, kept[k], passed[k])[0]
            arrived.append(split_swap(both, (2, 1)))
        own = call(
            functools.partial(own_kernel, tile), [((per_group, cells), full)], [FULL] * 2, weight, damage
        )[0]
    else:
        every = [scores] + [swap(scores, "grp", step) for step in range(1, groups)]
        own, *parts = call(
            functools.partial(direct_kernel, groups, min(cells, 512)),
            [((per_group, cells), full)] + [part] * (groups - 1),
            [FULL] * (2 + groups),
            picks,
            damage,
            *every,
            scratch=[pltpu.VMEM((samples, rows), half)],
            limit=32,
        )
        arrived = [swap(x, "grp", step) for step, x in enumerate(parts, 1)]

    values, stats = call(
        values_kernel,
        [((per_group, cells), full), ((2, per_group), full)],
        [FULL] * (1 + len(arrived)),
        own,
        *arrived,
    )
    surrogate = call(round_kernel, [part], [FULL], values)[0]
    squares, peak = over_nodes(stats, nodes)
    spread = jnp.sqrt(squares / (cells * nodes) + 1e-06)
    return (surrogate, peak, spread)


def split_columns(cells):
    late = cells // 4
    return cells - late, late


def is_paired(groups, nodes):
    return groups == 4 and nodes % 2 == 0


def solution(mesh):
    placed = (P("grp", "node"), P("grp", None), P("grp"), P(), P(), P())
    return jax.shard_map(
        local,
        mesh=mesh,
        in_specs=placed,
        out_specs=(P("grp", "node"), P("grp"), P("grp")),
        check_vma=False,
    )
```

```python
import functools
import math

import jax
import jax.numpy as jnp
from jax import lax
from jax.experimental import pallas as pl
from jax.experimental.pallas import tpu as pltpu
from jax.sharding import PartitionSpec as P


FULL = pl.BlockSpec(memory_space=pltpu.VMEM)
FAR = pl.BlockSpec(memory_space=pltpu.HBM)


def mate(index, step, size):
    return index ^ step if size & (size - 1) == 0 else (index + step) % size


def origin(index, step, size):
    return index ^ step if size & (size - 1) == 0 else (index - step) % size


def swap(value, axis, step):
    size = lax.axis_size(axis)
    return lax.ppermute(value, axis, [(i, mate(i, step, size)) for i in range(size)])


def split_swap(value, steps):
    nodes = lax.axis_size("node")
    pairs = [
        (group * nodes + node, (group ^ steps[node % 2]) * nodes + node)
        for group in range(lax.axis_size("grp"))
        for node in range(nodes)
    ]
    return lax.ppermute(value, ("grp", "node"), pairs)


def node_swap(value, steps):
    pairs = [(node, node ^ steps[node % 2]) for node in range(lax.axis_size("node"))]
    return lax.ppermute(value, "node", pairs)


def scores_kernel(groups, table_ref, ids_ref, basis_ref, train_ref, counts_ref, damage_ref, *refs):
    (scores, named, damage), sends = refs[:3], refs[3:-7]
    table, ids, basis, train, counts, choice, sems = refs[-7:]
    pairs = (
        (ids_ref, ids),
        (table_ref, table),
        (basis_ref, basis),
        (counts_ref, counts),
        (train_ref, train),
        (damage_ref, damage),
    )
    copies = [pltpu.make_async_copy(src, dst, sems.at[k]) for k, (src, dst) in enumerate(pairs)]
    for copy in copies:
        copy.start()
    me = lax.axis_index("grp")
    samples = ids.shape[1]
    copies[0].wait()
    lane = lax.broadcasted_iota(jnp.int32, (samples, 128), 1)
    wanted = jnp.transpose(jnp.broadcast_to(ids[...].astype(jnp.float32), (128, samples)))
    for start in range(0, table.shape[0], 128):
        match = wanted == (lane + start).astype(jnp.float32)
        choice[:, start : start + 128] = match.astype(jnp.bfloat16)
    copies[1].wait()
    chosen = jnp.dot(choice[...], table[...], preferred_element_type=jnp.float32)
    copies[2].wait()
    found = lax.dot_general(
        chosen.astype(jnp.bfloat16),
        basis[...],
        (((1,), (1,)), ((), ())),
        preferred_element_type=jnp.float32,
    )
    copies[3].wait()
    total = lax.fori_loop(0, groups, lambda k, s: s + counts[k], jnp.int32(0)).astype(jnp.float32)
    scores[...] = (found * (1.0 / total)).astype(jnp.bfloat16)
    if sends:
        odd = lax.axis_index("node") % 2
        near_head, near_tail, side_head, side_tail = sends
        per_group = near_head.shape[0]
        other = me ^ (2 + odd)
        near_head[...] = rows_of(scores, other ^ 3, per_group)
        for place, step in enumerate((1, 2, 0)):
            near_tail[place * per_group : (place + 1) * per_group, :] = rows_of(
                scores, other ^ step, per_group
            )
        side_head[...] = rows_of(scores, me ^ 2, per_group)
        for place, step in enumerate((1, 2, 0)):
            side_tail[place * per_group : (place + 1) * per_group, :] = rows_of(
                scores, me ^ 1 ^ step, per_group
            )
    copies[4].wait()
    live = lax.broadcasted_iota(jnp.int32, named.shape, 1) < counts[me]
    named[...] = jnp.where(live, train[...], -1)
    copies[5].wait()


def rows_of(ref, block, rows):
    return ref[pl.ds(pl.multiple_of(block * rows, rows), rows), :]


def picks_kernel(groups, named_ref, out_ref):
    me = lax.axis_index("grp")
    row = lax.broadcasted_iota(jnp.int32, out_ref.shape[1:], 0)
    for step in range(groups):
        first = origin(me, step, groups) * out_ref.shape[1]
        out_ref[step] = jnp.where(row == named_ref[...] - first, 1.0, 0.0).astype(out_ref.dtype)


def project(weight, damage_ref, start, outs, tile):
    rows = weight.shape[0] // len(outs)
    for at in range(0, outs[0].shape[1], tile):
        part = jnp.dot(
            weight,
            damage_ref[:, start + at : start + at + tile],
            preferred_element_type=jnp.float32,
        )
        for k, out in enumerate(outs):
            out[:, at : at + tile] = part[k * rows : (k + 1) * rows, :].astype(out.dtype)


def first_kernel(tile, picks_ref, damage_ref, own, near, mated, side, weight, out):
    odd = lax.axis_index("node") % 2
    total = jnp.dot(
        rows_of(own, lax.axis_index("grp") ^ 3, near.shape[0]),
        picks_ref[0],
        preferred_element_type=jnp.float32,
    )
    for ref, step in ((near, 2 + odd), (mated, 3 - odd), (side, 1)):
        total += jnp.dot(ref[...], picks_ref[step], preferred_element_type=jnp.float32)
    weight[...] = total.astype(weight.dtype)
    project(weight[...], damage_ref, 0, [out], tile)


def second_kernel(tile, weight_ref, damage_ref, out_ref):
    project(weight_ref[...], damage_ref, damage_ref.shape[1] - out_ref.shape[1], [out_ref], tile)


def other_kernel(tile, picks_ref, damage_ref, own, near, mated, side, *refs):
    sent, kept, later, weight, order = refs
    odd = lax.axis_index("node") % 2
    me = lax.axis_index("grp")
    rows = sent.shape[0]
    steps = (2 - odd, 1 + odd, 0)
    total = None
    for ref, step in ((own, 0), (near, 2 + odd), (mated, 3 - odd), (side, 1)):
        for place, target in enumerate(steps):
            block = me ^ target if ref is own else (1 - odd, odd, 2)[place]
            order[place * rows : (place + 1) * rows, :] = rows_of(ref, block, rows)
        part = jnp.dot(order[...], picks_ref[step], preferred_element_type=jnp.float32)
        total = part if total is None else total + part
    total = total.astype(jnp.bfloat16)
    weight[...] = total[2 * rows :, :]
    for start, keep in ((0, kept), (kept.shape[1], later)):
        for at in range(0, keep.shape[1], tile):
            part = jnp.dot(
                total[: 2 * rows, :],
                damage_ref[:, start + at : start + at + tile],
                preferred_element_type=jnp.float32,
            )
            sent[:, start + at : start + at + tile] = part[:rows, :].astype(sent.dtype)
            keep[:, at : at + tile] = part[rows:, :]


def direct_kernel(groups, tile, picks_ref, damage_ref, *refs):
    scores, outs, order = refs[:groups], refs[groups:-1], refs[-1]
    me = lax.axis_index("grp")
    rows = outs[0].shape[0]
    total = None
    for step in range(groups):
        for target in range(groups):
            order[target * rows : (target + 1) * rows, :] = rows_of(
                scores[step], mate(me, target, groups), rows
            )
        part = jnp.dot(order[...], picks_ref[step], preferred_element_type=jnp.float32)
        total = part if total is None else total + part
    project(total.astype(jnp.bfloat16), damage_ref, 0, outs, tile)


def own_kernel(tile, weight_ref, damage_ref, out_ref):
    project(weight_ref[...], damage_ref, 0, [out_ref], tile)


def add_kernel(one_ref, two_ref, out_ref):
    out_ref[...] = (one_ref[...] + two_ref[...].astype(jnp.float32)).astype(out_ref.dtype)


def values_kernel(own_ref, *refs):
    parts, (out_ref, stats_ref) = refs[:-2], refs[-2:]
    rows, cells = out_ref.shape
    square = peak = None
    width = math.gcd(512, *[part.shape[1] for part in parts])
    for start in range(0, cells, width):
        values = own_ref[:, start : start + width]
        place = 0
        for part in parts:
            if place <= start < place + part.shape[1]:
                values = values + part[:, start - place : start - place + width].astype(jnp.float32)
            place = (place + part.shape[1]) % cells
        out_ref[:, start : start + width] = values
        more = jnp.sum(values * values, axis=1, keepdims=True)
        high = jnp.max(values, axis=1, keepdims=True)
        square = more if square is None else square + more
        peak = high if peak is None else jnp.maximum(peak, high)
    stats_ref[0:1, :] = jnp.transpose(jnp.broadcast_to(square, (rows, 128)))[0:1, :]
    stats_ref[1:2, :] = jnp.transpose(jnp.broadcast_to(peak, (rows, 128)))[0:1, :]


def round_kernel(values_ref, out_ref):
    out_ref[...] = values_ref[...].astype(out_ref.dtype)


def combine(first, second):
    return jnp.stack([first[0] + second[0], jnp.maximum(first[1], second[1])])


def over_nodes(stats, nodes):
    if nodes & (nodes - 1):
        everything = lax.all_gather(stats, "node")
        return jnp.stack([jnp.sum(everything[:, 0], axis=0), jnp.max(everything[:, 1], axis=0)])
    if nodes == 8:
        pair = combine(stats, node_swap(stats, (1, 1)))
        across = node_swap(pair, (4, 6))
        beside = node_swap(pair, (2, 2))
        return combine(combine(pair, beside), combine(across, node_swap(across, (1, 1))))
    step = 1
    while step < nodes:
        stats = combine(stats, swap(stats, "node", step))
        step *= 2
    return stats


def call(kernel, outs, ins, *args, scratch=(), limit=24):
    return pl.pallas_call(
        kernel,
        out_shape=[jax.ShapeDtypeStruct(shape, kind) for shape, kind in outs],
        in_specs=ins,
        out_specs=[FULL] * len(outs),
        scratch_shapes=list(scratch),
        compiler_params=pltpu.CompilerParams(vmem_limit_bytes=limit << 20),
        cost_estimate=pl.CostEstimate(flops=1 << 20, bytes_accessed=1 << 20, transcendentals=0),
    )(*args)


def local(damage, basis_table, train_ids, counts, new_table, new_ids):
    slots, cells = damage.shape
    groups = lax.axis_size("grp")
    nodes = lax.axis_size("node")
    samples = new_ids.shape[0]
    per_group = samples // groups
    rows = basis_table.shape[0]
    half, full = jnp.bfloat16, jnp.float32
    paired = is_paired(groups, nodes)
    operands = (new_table, new_ids.reshape(1, samples), basis_table, train_ids.reshape(1, slots), counts, damage)
    rest = samples - per_group
    sends = [(per_group, rows), (rest, rows)] * 2
    scores, named, damage, *sends = call(
        functools.partial(scores_kernel, groups),
        [((samples, rows), half), ((1, slots), jnp.int32), ((slots, cells), half)]
        + ([(shape, half) for shape in sends] if paired else []),
        [FAR] * 6,
        *[pltpu.with_memory_space_constraint(x, pltpu.HBM) for x in operands],
        scratch=[
            pltpu.VMEM(new_table.shape, half),
            pltpu.VMEM((1, samples), jnp.int32),
            pltpu.VMEM(basis_table.shape, half),
            pltpu.VMEM((1, slots), jnp.int32),
            pltpu.SMEM((groups,), jnp.int32),
            pltpu.VMEM((samples, new_table.shape[0]), half),
            pltpu.SemaphoreType.DMA((6,)),
        ],
        limit=32,
    )
    picks = call(
        functools.partial(picks_kernel, groups), [((groups, rows, slots), half)], [FULL], named
    )[0]
    part = ((per_group, cells), half)

    if paired:
        widths = split_columns(cells)
        tile = math.gcd(512, *widths)
        pieces = [(per_group, width) for width in widths]
        near_head, near_tail, side_head, side_tail = sends
        side_head = swap(side_head, "grp", 1)
        near_head = split_swap(near_head, (2, 3))
        side_tail = swap(side_tail, "grp", 1)
        near_tail = split_swap(near_tail, (2, 3))
        heads = (near_head, swap(near_head, "node", 1), side_head)
        tails = (near_tail, swap(near_tail, "node", 1), side_tail)
        weight, first = call(
            functools.partial(first_kernel, tile),
            [((per_group, slots), half), (pieces[0], half)],
            [FULL] * 6,
            picks,
            damage,
            scores,
            *heads,
        )
        second = call(
            functools.partial(second_kernel, tile), [(pieces[1], half)], [FULL] * 2, weight, damage
        )[0]
        passed = [split_swap(x, (2, 1)) for x in (first, second)]
        sent, *kept, weight = call(
            functools.partial(other_kernel, tile),
            [part, (pieces[0], full), (pieces[1], full), ((per_group, slots), half)],
            [FULL] * 6,
            picks,
            damage,
            scores,
            *tails,
            scratch=[pltpu.VMEM((rest, rows), half)],
        )
        arrived = [split_swap(sent, (2, 1))]
        for k in range(2):
            both = call(add_kernel, [(pieces[k], half)], [FULL] * 2, kept[k], passed[k])[0]
            arrived.append(split_swap(both, (1, 2)))
        own = call(
            functools.partial(own_kernel, tile), [((per_group, cells), full)], [FULL] * 2, weight, damage
        )[0]
    else:
        every = [scores] + [swap(scores, "grp", step) for step in range(1, groups)]
        own, *parts = call(
            functools.partial(direct_kernel, groups, min(cells, 512)),
            [((per_group, cells), full)] + [part] * (groups - 1),
            [FULL] * (2 + groups),
            picks,
            damage,
            *every,
            scratch=[pltpu.VMEM((samples, rows), half)],
            limit=32,
        )
        arrived = [swap(x, "grp", step) for step, x in enumerate(parts, 1)]

    values, stats = call(
        values_kernel,
        [((per_group, cells), full), ((2, per_group), full)],
        [FULL] * (1 + len(arrived)),
        own,
        *arrived,
    )
    surrogate = call(round_kernel, [part], [FULL], values)[0]
    squares, peak = over_nodes(stats, nodes)
    spread = jnp.sqrt(squares / (cells * nodes) + 1e-06)
    return (surrogate, peak, spread)


def split_columns(cells):
    late = 3 * cells // 8
    return cells - late, late


def is_paired(groups, nodes):
    return groups == 4 and nodes % 2 == 0


def solution(mesh):
    placed = (P("grp", "node"), P("grp", None), P("grp"), P(), P(), P())
    return jax.shard_map(
        local,
        mesh=mesh,
        in_specs=placed,
        out_specs=(P("grp", "node"), P("grp"), P("grp")),
        check_vma=False,
    )
```

```python
import functools
import math

import jax
import jax.numpy as jnp
from jax import lax
from jax.experimental import pallas as pl
from jax.experimental.pallas import tpu as pltpu
from jax.sharding import PartitionSpec as P


FULL = pl.BlockSpec(memory_space=pltpu.VMEM)
FAR = pl.BlockSpec(memory_space=pltpu.HBM)


def mate(index, step, size):
    return index ^ step if size & (size - 1) == 0 else (index + step) % size


def origin(index, step, size):
    return index ^ step if size & (size - 1) == 0 else (index - step) % size


def swap(value, axis, step):
    size = lax.axis_size(axis)
    return lax.ppermute(value, axis, [(i, mate(i, step, size)) for i in range(size)])


def split_swap(value, steps):
    nodes = lax.axis_size("node")
    pairs = [
        (group * nodes + node, (group ^ steps[node % 2]) * nodes + node)
        for group in range(lax.axis_size("grp"))
        for node in range(nodes)
    ]
    return lax.ppermute(value, ("grp", "node"), pairs)


def node_swap(value, steps):
    pairs = [(node, node ^ steps[node % 2]) for node in range(lax.axis_size("node"))]
    return lax.ppermute(value, "node", pairs)


def scores_kernel(groups, table_ref, ids_ref, basis_ref, train_ref, counts_ref, damage_ref, *refs):
    (scores, named, damage), sends = refs[:3], refs[3:-7]
    table, ids, basis, train, counts, choice, sems = refs[-7:]
    pairs = (
        (ids_ref, ids),
        (table_ref, table),
        (basis_ref, basis),
        (counts_ref, counts),
        (train_ref, train),
        (damage_ref, damage),
    )
    copies = [pltpu.make_async_copy(src, dst, sems.at[k]) for k, (src, dst) in enumerate(pairs)]
    for copy in copies:
        copy.start()
    me = lax.axis_index("grp")
    samples = ids.shape[1]
    copies[0].wait()
    lane = lax.broadcasted_iota(jnp.int32, (samples, 128), 1)
    wanted = jnp.transpose(jnp.broadcast_to(ids[...].astype(jnp.float32), (128, samples)))
    for start in range(0, table.shape[0], 128):
        match = wanted == (lane + start).astype(jnp.float32)
        choice[:, start : start + 128] = match.astype(jnp.bfloat16)
    copies[1].wait()
    chosen = jnp.dot(choice[...], table[...], preferred_element_type=jnp.float32)
    copies[2].wait()
    found = lax.dot_general(
        chosen.astype(jnp.bfloat16),
        basis[...],
        (((1,), (1,)), ((), ())),
        preferred_element_type=jnp.float32,
    )
    copies[3].wait()
    total = lax.fori_loop(0, groups, lambda k, s: s + counts[k], jnp.int32(0)).astype(jnp.float32)
    scores[...] = (found * (1.0 / total)).astype(jnp.bfloat16)
    if sends:
        odd = lax.axis_index("node") % 2
        near_head, near_tail, side_head, side_tail = sends
        per_group = near_head.shape[0]
        other = me ^ (2 + odd)
        near_head[...] = rows_of(scores, other ^ 3, per_group)
        for place, step in enumerate((1, 2, 0)):
            near_tail[place * per_group : (place + 1) * per_group, :] = rows_of(
                scores, other ^ step, per_group
            )
        side_head[...] = rows_of(scores, me ^ 2, per_group)
        for place, step in enumerate((1, 2, 0)):
            side_tail[place * per_group : (place + 1) * per_group, :] = rows_of(
                scores, me ^ 1 ^ step, per_group
            )
    copies[4].wait()
    live = lax.broadcasted_iota(jnp.int32, named.shape, 1) < counts[me]
    named[...] = jnp.where(live, train[...], -1)
    copies[5].wait()


def rows_of(ref, block, rows):
    return ref[pl.ds(pl.multiple_of(block * rows, rows), rows), :]


def picks_kernel(groups, named_ref, out_ref):
    me = lax.axis_index("grp")
    row = lax.broadcasted_iota(jnp.int32, out_ref.shape[1:], 0)
    for step in range(groups):
        first = origin(me, step, groups) * out_ref.shape[1]
        out_ref[step] = jnp.where(row == named_ref[...] - first, 1.0, 0.0).astype(out_ref.dtype)


def project(weight, damage_ref, start, outs, tile):
    rows = weight.shape[0] // len(outs)
    for at in range(0, outs[0].shape[1], tile):
        part = jnp.dot(
            weight,
            damage_ref[:, start + at : start + at + tile],
            preferred_element_type=jnp.float32,
        )
        for k, out in enumerate(outs):
            out[:, at : at + tile] = part[k * rows : (k + 1) * rows, :].astype(out.dtype)


def early_kernel(picks_ref, own, near, weight):
    odd = lax.axis_index("node") % 2
    weight[...] = jnp.dot(
        rows_of(own, lax.axis_index("grp") ^ 3, near.shape[0]),
        picks_ref[0],
        preferred_element_type=jnp.float32,
    ) + jnp.dot(near[...], picks_ref[2 + odd], preferred_element_type=jnp.float32)


def first_kernel(tile, picks_ref, damage_ref, early, mated, side, weight, out):
    odd = lax.axis_index("node") % 2
    total = early[...]
    for ref, step in ((mated, 3 - odd), (side, 1)):
        total += jnp.dot(ref[...], picks_ref[step], preferred_element_type=jnp.float32)
    weight[...] = total.astype(weight.dtype)
    project(weight[...], damage_ref, 0, [out], tile)


def second_kernel(tile, weight_ref, damage_ref, out_ref):
    project(weight_ref[...], damage_ref, damage_ref.shape[1] - out_ref.shape[1], [out_ref], tile)


def other_kernel(tile, picks_ref, damage_ref, own, near, mated, side, *refs):
    sent, kept, later, weight, order = refs
    odd = lax.axis_index("node") % 2
    me = lax.axis_index("grp")
    rows = sent.shape[0]
    steps = (2 - odd, 1 + odd, 0)
    total = None
    for ref, step in ((own, 0), (near, 2 + odd), (mated, 3 - odd), (side, 1)):
        for place, target in enumerate(steps):
            block = me ^ target if ref is own else (1 - odd, odd, 2)[place]
            order[place * rows : (place + 1) * rows, :] = rows_of(ref, block, rows)
        part = jnp.dot(order[...], picks_ref[step], preferred_element_type=jnp.float32)
        total = part if total is None else total + part
    total = total.astype(jnp.bfloat16)
    weight[...] = total[2 * rows :, :]
    for start, keep in ((0, kept), (kept.shape[1], later)):
        for at in range(0, keep.shape[1], tile):
            part = jnp.dot(
                total[: 2 * rows, :],
                damage_ref[:, start + at : start + at + tile],
                preferred_element_type=jnp.float32,
            )
            sent[:, start + at : start + at + tile] = part[:rows, :].astype(sent.dtype)
            keep[:, at : at + tile] = part[rows:, :]


def direct_kernel(groups, tile, picks_ref, damage_ref, *refs):
    scores, outs, order = refs[:groups], refs[groups:-1], refs[-1]
    me = lax.axis_index("grp")
    rows = outs[0].shape[0]
    total = None
    for step in range(groups):
        for target in range(groups):
            order[target * rows : (target + 1) * rows, :] = rows_of(
                scores[step], mate(me, target, groups), rows
            )
        part = jnp.dot(order[...], picks_ref[step], preferred_element_type=jnp.float32)
        total = part if total is None else total + part
    project(total.astype(jnp.bfloat16), damage_ref, 0, outs, tile)


def own_kernel(tile, weight_ref, damage_ref, out_ref):
    project(weight_ref[...], damage_ref, 0, [out_ref], tile)


def add_kernel(one_ref, two_ref, out_ref):
    out_ref[...] = (one_ref[...] + two_ref[...].astype(jnp.float32)).astype(out_ref.dtype)


def values_kernel(own_ref, *refs):
    parts, (out_ref, stats_ref) = refs[:-2], refs[-2:]
    rows, cells = out_ref.shape
    square = peak = None
    width = math.gcd(512, *[part.shape[1] for part in parts])
    for start in range(0, cells, width):
        values = own_ref[:, start : start + width]
        place = 0
        for part in parts:
            if place <= start < place + part.shape[1]:
                values = values + part[:, start - place : start - place + width].astype(jnp.float32)
            place = (place + part.shape[1]) % cells
        out_ref[:, start : start + width] = values
        more = jnp.sum(values * values, axis=1, keepdims=True)
        high = jnp.max(values, axis=1, keepdims=True)
        square = more if square is None else square + more
        peak = high if peak is None else jnp.maximum(peak, high)
    stats_ref[0:1, :] = jnp.transpose(jnp.broadcast_to(square, (rows, 128)))[0:1, :]
    stats_ref[1:2, :] = jnp.transpose(jnp.broadcast_to(peak, (rows, 128)))[0:1, :]


def round_kernel(values_ref, out_ref):
    out_ref[...] = values_ref[...].astype(out_ref.dtype)


def combine(first, second):
    return jnp.stack([first[0] + second[0], jnp.maximum(first[1], second[1])])


def over_nodes(stats, nodes):
    if nodes & (nodes - 1):
        everything = lax.all_gather(stats, "node")
        return jnp.stack([jnp.sum(everything[:, 0], axis=0), jnp.max(everything[:, 1], axis=0)])
    if nodes == 8:
        pair = combine(stats, node_swap(stats, (1, 1)))
        across = node_swap(pair, (4, 6))
        beside = node_swap(pair, (2, 2))
        return combine(combine(pair, beside), combine(across, node_swap(across, (1, 1))))
    step = 1
    while step < nodes:
        stats = combine(stats, swap(stats, "node", step))
        step *= 2
    return stats


def call(kernel, outs, ins, *args, scratch=(), limit=24):
    return pl.pallas_call(
        kernel,
        out_shape=[jax.ShapeDtypeStruct(shape, kind) for shape, kind in outs],
        in_specs=ins,
        out_specs=[FULL] * len(outs),
        scratch_shapes=list(scratch),
        compiler_params=pltpu.CompilerParams(vmem_limit_bytes=limit << 20),
        cost_estimate=pl.CostEstimate(flops=1 << 20, bytes_accessed=1 << 20, transcendentals=0),
    )(*args)


def local(damage, basis_table, train_ids, counts, new_table, new_ids):
    slots, cells = damage.shape
    groups = lax.axis_size("grp")
    nodes = lax.axis_size("node")
    samples = new_ids.shape[0]
    per_group = samples // groups
    rows = basis_table.shape[0]
    half, full = jnp.bfloat16, jnp.float32
    paired = is_paired(groups, nodes)
    operands = (new_table, new_ids.reshape(1, samples), basis_table, train_ids.reshape(1, slots), counts, damage)
    rest = samples - per_group
    sends = [(per_group, rows), (rest, rows)] * 2
    scores, named, damage, *sends = call(
        functools.partial(scores_kernel, groups),
        [((samples, rows), half), ((1, slots), jnp.int32), ((slots, cells), half)]
        + ([(shape, half) for shape in sends] if paired else []),
        [FAR] * 6,
        *[pltpu.with_memory_space_constraint(x, pltpu.HBM) for x in operands],
        scratch=[
            pltpu.VMEM(new_table.shape, half),
            pltpu.VMEM((1, samples), jnp.int32),
            pltpu.VMEM(basis_table.shape, half),
            pltpu.VMEM((1, slots), jnp.int32),
            pltpu.SMEM((groups,), jnp.int32),
            pltpu.VMEM((samples, new_table.shape[0]), half),
            pltpu.SemaphoreType.DMA((6,)),
        ],
        limit=32,
    )
    picks = call(functools.partial(picks_kernel, groups), [((groups, rows, slots), half)], [FULL], named)[0]
    part = ((per_group, cells), half)

    if paired:
        widths = split_columns(cells)
        tile = math.gcd(512, *widths)
        pieces = [(per_group, width) for width in widths]
        near_head, near_tail, side_head, side_tail = sends
        side_head = swap(side_head, "grp", 1)
        near_head = split_swap(near_head, (2, 3))
        side_tail = swap(side_tail, "grp", 1)
        near_tail = split_swap(near_tail, (2, 3))
        heads = (near_head, swap(near_head, "node", 1), side_head)
        tails = (near_tail, swap(near_tail, "node", 1), side_tail)
        early = call(early_kernel, [((per_group, slots), full)], [FULL] * 3, picks, scores, near_head)[0]
        weight, first = call(
            functools.partial(first_kernel, tile),
            [((per_group, slots), half), (pieces[0], half)],
            [FULL] * 5,
            picks,
            damage,
            early,
            *heads[1:],
        )
        second = call(functools.partial(second_kernel, tile), [(pieces[1], half)], [FULL] * 2, weight, damage)[0]
        passed = [split_swap(x, (2, 1)) for x in (first, second)]
        sent, *kept, weight = call(
            functools.partial(other_kernel, tile),
            [part, (pieces[0], full), (pieces[1], full), ((per_group, slots), half)],
            [FULL] * 6,
            picks,
            damage,
            scores,
            *tails,
            scratch=[pltpu.VMEM((rest, rows), half)],
        )
        arrived = [split_swap(sent, (2, 1))]
        for k in range(2):
            both = call(add_kernel, [(pieces[k], half)], [FULL] * 2, kept[k], passed[k])[0]
            arrived.append(split_swap(both, (1, 2)))
        own = call(functools.partial(own_kernel, tile), [((per_group, cells), full)], [FULL] * 2, weight, damage)[0]
    else:
        every = [scores] + [swap(scores, "grp", step) for step in range(1, groups)]
        own, *parts = call(
            functools.partial(direct_kernel, groups, min(cells, 512)),
            [((per_group, cells), full)] + [part] * (groups - 1),
            [FULL] * (2 + groups),
            picks,
            damage,
            *every,
            scratch=[pltpu.VMEM((samples, rows), half)],
            limit=32,
        )
        arrived = [swap(x, "grp", step) for step, x in enumerate(parts, 1)]

    values, stats = call(
        values_kernel, [((per_group, cells), full), ((2, per_group), full)], [FULL] * (1 + len(arrived)), own, *arrived
    )
    surrogate = call(round_kernel, [part], [FULL], values)[0]
    squares, peak = over_nodes(stats, nodes)
    spread = jnp.sqrt(squares / (cells * nodes) + 1e-06)
    return (surrogate, peak, spread)


def split_columns(cells):
    late = 3 * cells // 8
    return cells - late, late


def is_paired(groups, nodes):
    return groups == 4 and nodes % 2 == 0


def solution(mesh):
    placed = (P("grp", "node"), P("grp", None), P("grp"), P(), P(), P())
    return jax.shard_map(
        local,
        mesh=mesh,
        in_specs=placed,
        out_specs=(P("grp", "node"), P("grp"), P("grp")),
        check_vma=False,
    )
```
